16 devices in a mesh: dp: 2 (over y, z), sp: 8 (over x, core).
Axes of the slice: x: 4, y: 2, z: 1, core: 2. Of those that a mesh axis runs over, the one named last changes fastest.
The devices are a block of a 4x4x8 slice.
Arguments:
- hidden: bfloat16 [256, 4544], P('dp'), parts along dimension 0
- ln_gamma: float32 [4544], replicated
- ln_beta: float32 [4544], replicated
- w_qkv: bfloat16 [4544, 4672], replicated
- w_out: bfloat16 [4544, 4544], replicated
- w_up: bfloat16 [4544, 18176], P(None, 'sp')
- w_down: bfloat16 [18176, 4544], P('sp')
- k_cache: bfloat16 [256, 8192, 64], P('dp', 'sp'), parts along dimension 0
- v_cache: bfloat16 [256, 8192, 64], P('dp', 'sp'), parts along dimension 0
- positions: int32 [256], P('dp'), parts along dimension 0
Outputs:
- output 1: bfloat16 [256, 4544], P('dp'), parts along dimension 0
- output 2: bfloat16 [256, 8192, 64], P('dp', 'sp'), parts along dimension 0
- output 3: bfloat16 [256, 8192, 64], P('dp', 'sp'), parts along dimension 0
There are 2 independent parts. The reference program is written for one: setup_inputs(seed, part) draws one part's arguments, and reference() takes and returns one part's arrays. A program takes and returns all parts, laid end to end along the dimension named above; an argument that names none is the same for every part.
All inputs are finite; a program needn't handle non-finite values.
Results may differ from the reference program's by a relative error of at most 0.00624681.
Values sent between devices are 32-bit elements.
A program may use at most 768 MiB of HBM per device.

```python
import jax
import jax.numpy as jnp
from jax import lax

BATCH_ROWS = 128
D_MODEL = 4544
N_HEADS = 71
HEAD_DIM = 64
FF_DIM = 18176
SEQ_SHARD = 1024
N_SHARDS = 8
SEQ_LEN = N_SHARDS * SEQ_SHARD
LN_EPS = 1e-5
ROPE_BASE = 10000.0
NEG_FILL = -1e30


def setup_inputs(seed: int = 0, part: int = 0) -> dict:
    base_key = jax.random.key(seed)
    weight_keys = jax.random.split(base_key, 6)
    part_keys = jax.random.split(jax.random.fold_in(base_key, part), 4)
    hidden = jax.random.normal(part_keys[0], (BATCH_ROWS, D_MODEL), jnp.float32).astype(jnp.bfloat16)
    ln_gamma = 1.0 + 0.3 * jax.random.normal(weight_keys[0], (D_MODEL,), jnp.float32)
    ln_beta = 0.3 * jax.random.normal(weight_keys[1], (D_MODEL,), jnp.float32)
    w_qkv = (jax.random.normal(weight_keys[2], (D_MODEL, (N_HEADS + 2) * HEAD_DIM), jnp.float32) * D_MODEL ** -0.5).astype(jnp.bfloat16)
    out_scale = 0.5 * SEQ_LEN ** 0.5 * (N_HEADS * HEAD_DIM) ** -0.5
    w_out = (jax.random.normal(weight_keys[3], (N_HEADS * HEAD_DIM, D_MODEL), jnp.float32) * out_scale).astype(jnp.bfloat16)
    w_up = (jax.random.normal(weight_keys[4], (D_MODEL, FF_DIM), jnp.float32) * D_MODEL ** -0.5).astype(jnp.bfloat16)
    w_down = (jax.random.normal(weight_keys[5], (FF_DIM, D_MODEL), jnp.float32) * FF_DIM ** -0.5).astype(jnp.bfloat16)
    k_cache = jax.random.normal(part_keys[1], (BATCH_ROWS, SEQ_LEN, HEAD_DIM), jnp.float32).astype(jnp.bfloat16)
    v_cache = jax.random.normal(part_keys[2], (BATCH_ROWS, SEQ_LEN, HEAD_DIM), jnp.float32).astype(jnp.bfloat16)
    positions = jax.random.randint(part_keys[3], (BATCH_ROWS,), SEQ_LEN // 2, SEQ_LEN, dtype=jnp.int32)
    positions = positions.at[0].set(SEQ_LEN - 1).at[1].set(SEQ_LEN // 2)
    return {'hidden': hidden, 'ln_gamma': ln_gamma, 'ln_beta': ln_beta, 'w_qkv': w_qkv, 'w_out': w_out, 'w_up': w_up, 'w_down': w_down, 'k_cache': k_cache, 'v_cache': v_cache, 'positions': positions}


def layer_norm(hidden, ln_gamma, ln_beta):
    hidden_f32 = hidden.astype(jnp.float32)
    row_mean = jnp.mean(hidden_f32, axis=-1, keepdims=True)
    centered = hidden_f32 - row_mean
    row_var = jnp.mean(centered * centered, axis=-1, keepdims=True)
    return (centered * lax.rsqrt(row_var + LN_EPS) * ln_gamma + ln_beta).astype(jnp.bfloat16)


def rotary_tables(positions, head_dim):
    inv_freq = 1.0 / (ROPE_BASE ** (jnp.arange(0, head_dim, 2, dtype=jnp.float32) / head_dim))
    angles = positions.astype(jnp.float32)[:, None] * inv_freq[None, :]
    cos_half = jnp.cos(angles)
    sin_half = jnp.sin(angles)
    return jnp.concatenate([cos_half, cos_half], axis=-1), jnp.concatenate([sin_half, sin_half], axis=-1)


def apply_rotary(vecs, cos_full, sin_full):
    vecs_f32 = vecs.astype(jnp.float32)
    half_dim = vecs.shape[-1] // 2
    rotated = jnp.concatenate([-vecs_f32[..., half_dim:], vecs_f32[..., :half_dim]], axis=-1)
    return (vecs_f32 * cos_full + rotated * sin_full).astype(jnp.bfloat16)


def row_attention(row_inputs):
    q_row, k_row, v_row, pos_row = row_inputs
    scores = jnp.dot(q_row, k_row.T, preferred_element_type=jnp.float32) * HEAD_DIM ** -0.5
    scores = scores.reshape(N_HEADS, N_SHARDS, SEQ_SHARD)
    valid_mask = (jnp.arange(SEQ_LEN) <= pos_row).reshape(N_SHARDS, SEQ_SHARD)
    masked = jnp.where(valid_mask, scores, NEG_FILL)
    block_max = jnp.max(masked, axis=-1)
    exp_scores = jnp.where(valid_mask, jnp.exp(masked - block_max[..., None]), 0.0)
    block_sum = jnp.sum(exp_scores, axis=-1)
    block_ctx = jnp.einsum('hcs,csd->hcd', exp_scores.astype(jnp.bfloat16).astype(jnp.float32), v_row.reshape(N_SHARDS, SEQ_SHARD, HEAD_DIM).astype(jnp.float32))
    top_max = jnp.max(block_max, axis=-1)
    scale_w = jnp.exp(block_max - top_max[:, None])
    total_sum = jnp.sum(block_sum * scale_w, axis=-1)
    total_ctx = jnp.sum(block_ctx * scale_w[..., None], axis=1)
    return (total_ctx / total_sum[:, None]).astype(jnp.bfloat16)


def reference(hidden, ln_gamma, ln_beta, w_qkv, w_out, w_up, w_down, k_cache, v_cache, positions):
    normed = layer_norm(hidden, ln_gamma, ln_beta)
    qkv_proj = jnp.dot(normed, w_qkv, preferred_element_type=jnp.float32).astype(jnp.bfloat16)
    qkv_proj = qkv_proj.reshape(BATCH_ROWS, N_HEADS + 2, HEAD_DIM)
    cos_full, sin_full = rotary_tables(positions, HEAD_DIM)
    q_rot = apply_rotary(qkv_proj[:, :N_HEADS], cos_full[:, None, :], sin_full[:, None, :])
    k_rot = apply_rotary(qkv_proj[:, N_HEADS], cos_full, sin_full)
    v_new = qkv_proj[:, N_HEADS + 1]
    write_mask = (jnp.arange(SEQ_LEN)[None, :] == positions[:, None])[:, :, None]
    k_next = jnp.where(write_mask, k_rot[:, None, :], k_cache)
    v_next = jnp.where(write_mask, v_new[:, None, :], v_cache)
    context = lax.map(row_attention, (q_rot, k_next, v_next, positions))
    attn_out = jnp.dot(context.reshape(BATCH_ROWS, N_HEADS * HEAD_DIM), w_out, preferred_element_type=jnp.float32)
    up_proj = jnp.dot(normed, w_up, preferred_element_type=jnp.float32)
    activated = jax.nn.gelu(up_proj, approximate=False).astype(jnp.bfloat16)
    mlp_out = jnp.dot(activated, w_down, preferred_element_type=jnp.float32)
    out_hidden = (hidden.astype(jnp.float32) + attn_out + mlp_out).astype(jnp.bfloat16)
    return (out_hidden, k_next, v_next)
```

```python
import functools

import jax
import jax.numpy as jnp
from jax import lax
from jax.experimental import pallas as pl
from jax.experimental.pallas import tpu as pltpu
from jax.sharding import PartitionSpec as P

LN_EPS = 1e-5
ROPE_BASE = 10000.0
NEG_FILL = -1e30
LANES = 128
ROWS_PER_CHUNK = 4
SLOTS = 6
AHEAD = 4


def layer_norm(hidden, ln_gamma, ln_beta):
    hidden_f32 = hidden.astype(jnp.float32)
    row_mean = jnp.mean(hidden_f32, axis=-1, keepdims=True)
    centered = hidden_f32 - row_mean
    row_var = jnp.mean(centered * centered, axis=-1, keepdims=True)
    return (centered * lax.rsqrt(row_var + LN_EPS) * ln_gamma + ln_beta).astype(jnp.bfloat16)


def rotary_tables(positions, head_dim):
    inv_freq = 1.0 / (ROPE_BASE ** (jnp.arange(0, head_dim, 2, dtype=jnp.float32) / head_dim))
    angles = positions.astype(jnp.float32)[:, None] * inv_freq[None, :]
    cos_half = jnp.cos(angles)
    sin_half = jnp.sin(angles)
    reps = 2 * LANES // head_dim
    return jnp.concatenate([cos_half] * reps, axis=-1), jnp.concatenate([sin_half] * reps, axis=-1)


def attention_kernel(num_pairs, pos_ref, qkv_ref, cos_ref, sin_ref, k_in, v_in, k_out, v_out, stats_ref,
                     q_s, k_new, v_new, k_buf, v_buf, in_sem, out_sem):
    rows, dim = qkv_ref.shape[0], k_in.shape[1]
    seq = k_in.shape[2]
    heads = 2 * num_pairs
    chunks = rows // ROWS_PER_CHUNK
    own_rows = rows // stats_ref.shape[0]

    def copies(chunk, slot):
        window = pl.ds(chunk * ROWS_PER_CHUNK, ROWS_PER_CHUNK)
        return (pltpu.make_async_copy(k_in.at[window], k_buf.at[slot], in_sem.at[0, slot]),
                pltpu.make_async_copy(v_in.at[window], v_buf.at[slot], in_sem.at[1, slot]))

    def stores(chunk, slot):
        window = pl.ds(chunk * ROWS_PER_CHUNK, ROWS_PER_CHUNK)
        return (pltpu.make_async_copy(k_buf.at[slot], k_out.at[window], out_sem.at[0, slot]),
                pltpu.make_async_copy(v_buf.at[slot], v_out.at[window], out_sem.at[1, slot]))

    for chunk in range(AHEAD):
        for copy in copies(chunk, chunk):
            copy.start()

    lane = lax.broadcasted_iota(jnp.int32, (rows, LANES), 1)
    row = lax.broadcasted_iota(jnp.int32, (rows, LANES), 0)
    low = lane < dim
    first_half = lax.rem(lane, dim) < dim // 2
    mine = (lax.rem(row, 2) == 0) == low

    def rope(x):
        rot = jnp.where(first_half, -pltpu.roll(x, LANES - dim // 2, 1), pltpu.roll(x, dim // 2, 1))
        y = x * cos_ref[...] + rot * sin_ref[...]
        return y.astype(jnp.bfloat16).astype(jnp.float32)

    def prepare(pair, carry):
        x = qkv_ref[:, pl.ds(pl.multiple_of(pair * LANES, LANES), LANES)].astype(jnp.float32)
        y = rope(x) * dim ** -0.5
        swapped = pltpu.roll(y, dim, 1)
        base = pl.multiple_of(pair * 2 * rows, 2 * rows)
        q_s[pl.ds(base, rows), :] = jnp.where(mine, jnp.where(low, y, swapped), 0.0)
        q_s[pl.ds(base + rows, rows), :] = jnp.where(mine, jnp.where(low, swapped, y), 0.0)
        return carry

    lax.fori_loop(0, num_pairs, prepare, 0)
    last = (num_pairs - 1) * LANES
    k_new[...] = rope(qkv_ref[:, last:last + LANES].astype(jnp.float32)).T[dim:, :]
    v_new[...] = qkv_ref[:, last + LANES:last + LANES + dim].astype(jnp.float32).T

    dim_lane = lax.broadcasted_iota(jnp.int32, (dim, LANES), 1)
    slot_ids = lax.broadcasted_iota(jnp.int32, (1, seq), 1)
    head_lane = lax.broadcasted_iota(jnp.int32, (heads, LANES), 1)

    def step(chunk, carry):
        slot = lax.rem(chunk, SLOTS)
        for copy in copies(chunk, slot):
            copy.wait()
        for r in range(ROWS_PER_CHUNK):
            b = chunk * ROWS_PER_CHUNK + r
            at = pos_ref[b]

            @pl.when((at >= 0) & (at < seq))
            def _():
                start = pl.multiple_of((at // LANES) * LANES, LANES)
                hit = dim_lane == at - start
                for new, buf in ((k_new, k_buf), (v_new, v_buf)):
                    column = jnp.sum(jnp.where(dim_lane == b, new[...], 0.0), axis=1, keepdims=True)
                    old = buf[slot, r, :, pl.ds(start, LANES)].astype(jnp.float32)
                    buf[slot, r, :, pl.ds(start, LANES)] = jnp.where(hit, column, old).astype(jnp.bfloat16)

        for copy in stores(chunk, slot):
            copy.start()

        @pl.when(chunk + AHEAD < chunks)
        def _():
            ahead = lax.rem(chunk + AHEAD, SLOTS)

            @pl.when(chunk + AHEAD >= SLOTS)
            def _():
                for copy in stores(chunk + AHEAD - SLOTS, ahead):
                    copy.wait()

            for copy in copies(chunk + AHEAD, ahead):
                copy.start()

        owner = (chunk * ROWS_PER_CHUNK) // own_rows
        for half in range(ROWS_PER_CHUNK // 2):
            keys = k_buf[slot, 2 * half:2 * half + 2].reshape(2 * dim, seq)
            values = v_buf[slot, 2 * half:2 * half + 2].reshape(2 * dim, seq)
            parts = []
            for r in (2 * half, 2 * half + 1):
                b = chunk * ROWS_PER_CHUNK + r
                at = pos_ref[b]
                q = q_s[pl.ds(b, heads, stride=rows), :].astype(jnp.bfloat16)
                s = jnp.dot(q, keys, preferred_element_type=jnp.float32)
                s = jnp.where(slot_ids <= at, s, NEG_FILL)
                m = jnp.max(s, axis=1, keepdims=True)
                e = jnp.exp(s - jnp.where(at >= 0, m, 0.0))
                total = jnp.sum(e, axis=1, keepdims=True)
                o = lax.dot_general(e.astype(jnp.bfloat16), values, (((1,), (1,)), ((), ())),
                                    preferred_element_type=jnp.float32)
                parts.append(o)
                local = lax.rem(b, own_rows)
                table = stats_ref[owner, own_rows // 2]
                table = jnp.where(head_lane == local, m, jnp.where(head_lane == own_rows + local, total, table))
                stats_ref[owner, own_rows // 2] = table
            pair = lax.rem(chunk * ROWS_PER_CHUNK, own_rows) // 2 + half
            stats_ref[owner, pair] = jnp.where(head_lane < dim, parts[0], parts[1])
        return carry

    lax.fori_loop(0, chunks, step, 0)
    for chunk in range(chunks - SLOTS, chunks):
        for copy in stores(chunk, chunk % SLOTS):
            copy.wait()


def attention(local_pos, qkv, cos_full, sin_full, k_t, v_t, owners):
    rows, dim, seq = k_t.shape
    num_pairs = (qkv.shape[1] // dim - 1) // 2
    own_rows = rows // owners
    vmem = pl.BlockSpec(memory_space=pltpu.VMEM)
    hbm = pl.BlockSpec(memory_space=pl.ANY)
    return pl.pallas_call(
        functools.partial(attention_kernel, num_pairs),
        out_shape=(jax.ShapeDtypeStruct(k_t.shape, k_t.dtype), jax.ShapeDtypeStruct(v_t.shape, v_t.dtype),
                   jax.ShapeDtypeStruct((owners, own_rows // 2 + 1, 2 * num_pairs, LANES), jnp.float32)),
        in_specs=[pl.BlockSpec(memory_space=pltpu.SMEM), vmem, vmem, vmem, hbm, hbm],
        out_specs=(hbm, hbm, vmem),
        scratch_shapes=[
            pltpu.VMEM((2 * num_pairs * rows, LANES), jnp.float32),
            pltpu.VMEM((dim, LANES), jnp.float32),
            pltpu.VMEM((dim, LANES), jnp.float32),
            pltpu.VMEM((SLOTS, ROWS_PER_CHUNK, dim, seq), k_t.dtype),
            pltpu.VMEM((SLOTS, ROWS_PER_CHUNK, dim, seq), v_t.dtype),
            pltpu.SemaphoreType.DMA((2, SLOTS)),
            pltpu.SemaphoreType.DMA((2, SLOTS)),
        ],
        compiler_params=pltpu.CompilerParams(vmem_limit_bytes=48 * 2 ** 20),
        cost_estimate=pl.CostEstimate(flops=4 * rows * 2 * num_pairs * seq * dim, transcendentals=0,
                                      bytes_accessed=8 * rows * dim * seq),
    )(local_pos, qkv, cos_full, sin_full, k_t, v_t)


def combine(gathered, dim, heads):
    own_rows = (gathered.shape[1] - 1) * 2
    block_max = gathered[:, -1, :, :own_rows]
    block_sum = gathered[:, -1, :, own_rows:2 * own_rows]
    scale_w = jnp.exp(block_max - jnp.max(block_max, axis=0)[None])
    total_sum = jnp.sum(block_sum * scale_w, axis=0)
    sources, pairs, slots, _ = gathered[:, :-1].shape
    parts = gathered[:, :-1].reshape(sources, pairs, slots, 2, dim)
    weights = scale_w.reshape(sources, slots, pairs, 2).transpose(0, 2, 1, 3)
    total_ctx = jnp.sum(parts * weights[..., None], axis=0)
    ctx = total_ctx / total_sum.reshape(slots, pairs, 2).transpose(1, 0, 2)[..., None]
    ctx = ctx[:, :heads].transpose(0, 2, 1, 3).reshape(own_rows, heads * dim)
    return ctx.astype(jnp.bfloat16)


def device_step(hidden, ln_gamma, ln_beta, w_qkv, w_out, w_up, w_down, k_cache, v_cache, positions):
    seq_dev, head_dim = k_cache.shape[1], k_cache.shape[2]
    num_heads = w_out.shape[0] // head_dim
    group = lax.axis_size('sp')
    me = lax.axis_index('sp')
    normed = layer_norm(hidden, ln_gamma, ln_beta)
    qkv = jnp.dot(normed, w_qkv, preferred_element_type=jnp.float32).astype(jnp.bfloat16)
    cos_full, sin_full = rotary_tables(positions, head_dim)
    local_pos = positions - me * seq_dev
    k_t, v_t = jnp.swapaxes(k_cache, 1, 2), jnp.swapaxes(v_cache, 1, 2)
    k_next, v_next, stats = attention(local_pos, qkv, cos_full, sin_full, k_t, v_t, group)
    gathered = lax.all_to_all(stats, 'sp', 0, 0, tiled=True)
    context = combine(gathered, head_dim, num_heads)
    attn_out = jnp.dot(context, w_out, preferred_element_type=jnp.float32)
    up_proj = jnp.dot(normed, w_up, preferred_element_type=jnp.float32)
    activated = jax.nn.gelu(up_proj, approximate=False).astype(jnp.bfloat16)
    mlp_part = jnp.dot(activated, w_down, preferred_element_type=jnp.float32)
    mlp_own = lax.psum_scatter(mlp_part, 'sp', scatter_dimension=0, tiled=True)
    out_all = lax.all_gather(attn_out + mlp_own, 'sp', axis=0, tiled=True)
    out_hidden = (hidden.astype(jnp.float32) + out_all).astype(jnp.bfloat16)
    return out_hidden, jnp.swapaxes(k_next, 1, 2), jnp.swapaxes(v_next, 1, 2)


def solution(mesh):
    cache_spec = P('dp', 'sp', None)
    in_specs = (P('dp', None), P(None), P(None), P(None, None), P(None, None), P(None, 'sp'), P('sp', None), cache_spec, cache_spec, P('dp'))
    out_specs = (P('dp', None), cache_spec, cache_spec)
    return jax.shard_map(device_step, mesh=mesh, in_specs=in_specs, out_specs=out_specs, check_vma=False)
```

```python
import functools

import jax
import jax.numpy as jnp
from jax import lax
from jax.experimental import pallas as pl
from jax.experimental.pallas import tpu as pltpu
from jax.sharding import PartitionSpec as P

LN_EPS = 1e-5
ROPE_BASE = 10000.0
NEG_FILL = -1e30
LANES = 128
ROWS_PER_CHUNK = 8
SLOTS = 6
AHEAD = 4
PAD_ROWS = 8


def layer_norm(hidden, ln_gamma, ln_beta):
    hidden_f32 = hidden.astype(jnp.float32)
    row_mean = jnp.mean(hidden_f32, axis=-1, keepdims=True)
    centered = hidden_f32 - row_mean
    row_var = jnp.mean(centered * centered, axis=-1, keepdims=True)
    return (centered * lax.rsqrt(row_var + LN_EPS) * ln_gamma + ln_beta).astype(jnp.bfloat16)


def rotary_tables(positions, head_dim):
    inv_freq = 1.0 / (ROPE_BASE ** (jnp.arange(0, head_dim, 2, dtype=jnp.float32) / head_dim))
    angles = positions.astype(jnp.float32)[:, None] * inv_freq[None, :]
    cos_half = jnp.cos(angles)
    sin_half = jnp.sin(angles)
    reps = 2 * LANES // head_dim
    return jnp.concatenate([cos_half] * reps, axis=-1), jnp.concatenate([sin_half] * reps, axis=-1)


def attention_kernel(num_pairs, pos_ref, qkv_ref, cos_ref, sin_ref, k_in, v_in, k_out, v_out, stats_ref,
                     x_s, k_new, v_new, s_even, s_odd, e_even, e_odd, k_buf, v_buf, in_sem, out_sem):
    rows, dim = qkv_ref.shape[0], k_in.shape[1]
    seq = k_in.shape[2]
    heads = 2 * num_pairs
    stride = rows + PAD_ROWS
    chunks = rows // ROWS_PER_CHUNK
    own_rows = rows // stats_ref.shape[0]
    steps = ROWS_PER_CHUNK // 2
    full = num_pairs // 8 * 8
    tail = num_pairs - full

    def copies(chunk, slot):
        window = pl.ds(chunk * ROWS_PER_CHUNK, ROWS_PER_CHUNK)
        return (pltpu.make_async_copy(k_in.at[window], k_buf.at[slot], in_sem.at[0, slot]),
                pltpu.make_async_copy(v_in.at[window], v_buf.at[slot], in_sem.at[1, slot]))

    def stores(chunk, slot):
        window = pl.ds(chunk * ROWS_PER_CHUNK, ROWS_PER_CHUNK)
        return (pltpu.make_async_copy(k_buf.at[slot], k_out.at[window], out_sem.at[0, slot]),
                pltpu.make_async_copy(v_buf.at[slot], v_out.at[window], out_sem.at[1, slot]))

    for chunk in range(AHEAD):
        for copy in copies(chunk, chunk):
            copy.start()

    def rope(x, cos_full, sin_full):
        lane = lax.broadcasted_iota(jnp.int32, x.shape, 1)
        first_half = lax.rem(lane, dim) < dim // 2
        rot = jnp.where(first_half, -pltpu.roll(x, LANES - dim // 2, 1), pltpu.roll(x, dim // 2, 1))
        return (x * cos_full + rot * sin_full).astype(jnp.bfloat16).astype(jnp.float32)

    for pair in range(num_pairs):
        x_s[pair * stride:pair * stride + rows, :] = qkv_ref[:, pair * LANES:(pair + 1) * LANES].astype(jnp.float32)
    last = (num_pairs - 1) * LANES
    k_new[...] = rope(qkv_ref[:, last:last + LANES].astype(jnp.float32), cos_ref[...], sin_ref[...]).T[dim:, :]
    v_new[...] = qkv_ref[:, last + LANES:last + LANES + dim].astype(jnp.float32).T

    dim_lane = lax.broadcasted_iota(jnp.int32, (dim, LANES), 1)
    slot_ids = lax.broadcasted_iota(jnp.int32, (1, seq), 1)
    head_lane = lax.broadcasted_iota(jnp.int32, (heads, LANES), 1)
    tail_row = lax.broadcasted_iota(jnp.int32, (8, LANES), 0)
    scores = (s_even, s_odd)
    weights = (e_even, e_odd)

    def queries(b, low):
        x = x_s[pl.ds(b, full + 8, stride=stride), :]
        y = rope(x, cos_ref[pl.ds(b, 1), :], sin_ref[pl.ds(b, 1), :]) * dim ** -0.5
        z = pltpu.roll(y, dim, 1)
        first, second = (y, z) if low else (z, y)
        mixed = jnp.where(tail_row < tail, first[full:], pltpu.roll(second[full:], tail, 0))
        q = jnp.concatenate([first[:full], second[:full], mixed], axis=0)
        keep = (head_lane < dim) == low
        return jnp.where(keep, q, 0.0).astype(jnp.bfloat16)

    def score(chunk, slot, step):
        b = chunk * ROWS_PER_CHUNK + 2 * step
        keys = k_buf[slot, 2 * step:2 * step + 2].reshape(2 * dim, seq)
        q = jnp.concatenate([queries(b, True), queries(b + 1, False)], axis=0)
        s = jnp.dot(q, keys, preferred_element_type=jnp.float32)
        out = scores[step % 2]
        for r in range(2):
            out[r * heads:(r + 1) * heads, :] = jnp.where(slot_ids <= pos_ref[b + r], s[r * heads:(r + 1) * heads], NEG_FILL)

    def weigh(chunk, step):
        src, out = scores[step % 2], weights[step % 2]
        b = chunk * ROWS_PER_CHUNK + 2 * step
        owner = b // own_rows
        local = lax.rem(b, own_rows)
        table = stats_ref[owner, own_rows // 2]
        for r in range(2):
            s = src[r * heads:(r + 1) * heads, :]
            m = jnp.max(s, axis=1, keepdims=True)
            e = jnp.exp(s - jnp.where(pos_ref[b + r] >= 0, m, 0.0))
            total = jnp.sum(e, axis=1, keepdims=True)
            out[r * heads:(r + 1) * heads, :] = e.astype(jnp.bfloat16)
            table = jnp.where(head_lane == local + r, m,
                              jnp.where(head_lane == own_rows + local + r, total, table))
        stats_ref[owner, own_rows // 2] = table

    def apply(chunk, slot, step):
        b = chunk * ROWS_PER_CHUNK + 2 * step
        values = v_buf[slot, 2 * step:2 * step + 2].reshape(2 * dim, seq)
        o = lax.dot_general(weights[step % 2][...], values, (((1,), (1,)), ((), ())), preferred_element_type=jnp.float32)
        stats_ref[b // own_rows, lax.rem(b, own_rows) // 2] = jnp.where(head_lane < dim, o[:heads], o[heads:])

    def body(chunk, carry):
        slot = lax.rem(chunk, SLOTS)
        before = lax.rem(chunk + SLOTS - 1, SLOTS)
        earlier = jnp.maximum(chunk - 1, 0)
        for copy in copies(chunk, slot):
            copy.wait()
        for r in range(ROWS_PER_CHUNK):
            b = chunk * ROWS_PER_CHUNK + r
            at = pos_ref[b]

            @pl.when((at >= 0) & (at < seq))
            def _():
                start = pl.multiple_of((at // LANES) * LANES, LANES)
                hit = dim_lane == at - start
                for new, buf in ((k_new, k_buf), (v_new, v_buf)):
                    column = jnp.sum(jnp.where(dim_lane == b, new[...], 0.0), axis=1, keepdims=True)
                    old = buf[slot, r, :, pl.ds(start, LANES)].astype(jnp.float32)
                    buf[slot, r, :, pl.ds(start, LANES)] = jnp.where(hit, column, old).astype(jnp.bfloat16)

        for copy in stores(chunk, slot):
            copy.start()

        @pl.when(chunk + AHEAD < chunks)
        def _():
            ahead = lax.rem(chunk + AHEAD, SLOTS)

            @pl.when(chunk + AHEAD >= SLOTS)
            def _():
                for copy in stores(chunk + AHEAD - SLOTS, ahead):
                    copy.wait()

            for copy in copies(chunk + AHEAD, ahead):
                copy.start()

        for step in range(steps):
            if step >= 2:
                apply(chunk, slot, step - 2)
            else:
                apply(earlier, before, step - 2 + steps)
            score(chunk, slot, step)
            if step >= 1:
                weigh(chunk, step - 1)
            else:
                weigh(earlier, steps - 1)
        return carry

    lax.fori_loop(0, chunks, body, 0)
    apply(chunks - 1, (chunks - 1) % SLOTS, steps - 2)
    weigh(chunks - 1, steps - 1)
    apply(chunks - 1, (chunks - 1) % SLOTS, steps - 1)
    for chunk in range(chunks - SLOTS, chunks):
        for copy in stores(chunk, chunk % SLOTS):
            copy.wait()


def attention(local_pos, qkv, cos_full, sin_full, k_t, v_t, owners):
    rows, dim, seq = k_t.shape
    num_pairs = (qkv.shape[1] // dim - 1) // 2
    own_rows = rows // owners
    vmem = pl.BlockSpec(memory_space=pltpu.VMEM)
    hbm = pl.BlockSpec(memory_space=pl.ANY)
    return pl.pallas_call(
        functools.partial(attention_kernel, num_pairs),
        out_shape=(jax.ShapeDtypeStruct(k_t.shape, k_t.dtype), jax.ShapeDtypeStruct(v_t.shape, v_t.dtype),
                   jax.ShapeDtypeStruct((owners, own_rows // 2 + 1, 2 * num_pairs, LANES), jnp.float32)),
        in_specs=[pl.BlockSpec(memory_space=pltpu.SMEM), vmem, vmem, vmem, hbm, hbm],
        out_specs=(hbm, hbm, vmem),
        scratch_shapes=[
            pltpu.VMEM(((num_pairs // 8 * 8 + 8) * (rows + PAD_ROWS), LANES), jnp.float32),
            pltpu.VMEM((dim, LANES), jnp.float32),
            pltpu.VMEM((dim, LANES), jnp.float32),
            pltpu.VMEM((4 * num_pairs, seq), jnp.float32),
            pltpu.VMEM((4 * num_pairs, seq), jnp.float32),
            pltpu.VMEM((4 * num_pairs, seq), jnp.bfloat16),
            pltpu.VMEM((4 * num_pairs, seq), jnp.bfloat16),
            pltpu.VMEM((SLOTS, ROWS_PER_CHUNK, dim, seq), k_t.dtype),
            pltpu.VMEM((SLOTS, ROWS_PER_CHUNK, dim, seq), v_t.dtype),
            pltpu.SemaphoreType.DMA((2, SLOTS)),
            pltpu.SemaphoreType.DMA((2, SLOTS)),
        ],
        compiler_params=pltpu.CompilerParams(vmem_limit_bytes=48 * 2 ** 20),
        cost_estimate=pl.CostEstimate(flops=4 * rows * 2 * num_pairs * seq * dim, transcendentals=0,
                                      bytes_accessed=8 * rows * dim * seq),
    )(local_pos, qkv, cos_full, sin_full, k_t, v_t)


def combine(gathered, dim, heads):
    own_rows = (gathered.shape[1] - 1) * 2
    block_max = gathered[:, -1, :, :own_rows]
    block_sum = gathered[:, -1, :, own_rows:2 * own_rows]
    scale_w = jnp.exp(block_max - jnp.max(block_max, axis=0)[None])
    total_sum = jnp.sum(block_sum * scale_w, axis=0)
    sources, pairs, slots, _ = gathered[:, :-1].shape
    parts = gathered[:, :-1].reshape(sources, pairs, slots, 2, dim)
    weights = scale_w.reshape(sources, slots, pairs, 2).transpose(0, 2, 1, 3)
    total_ctx = jnp.sum(parts * weights[..., None], axis=0)
    ctx = total_ctx / total_sum.reshape(slots, pairs, 2).transpose(1, 0, 2)[..., None]
    full = slots // 16 * 8
    order = [h // 2 + (h % 2) * full if h < 2 * full else 2 * full + (h - 2 * full) // 2 + (h % 2) * (slots // 2 - full) for h in range(heads)]
    ctx = ctx[:, jnp.array(order)].transpose(0, 2, 1, 3).reshape(own_rows, heads * dim)
    return ctx.astype(jnp.bfloat16)


def device_step(hidden, ln_gamma, ln_beta, w_qkv, w_out, w_up, w_down, k_cache, v_cache, positions):
    seq_dev, head_dim = k_cache.shape[1], k_cache.shape[2]
    num_heads = w_out.shape[0] // head_dim
    group = lax.axis_size('sp')
    me = lax.axis_index('sp')
    normed = layer_norm(hidden, ln_gamma, ln_beta)
    qkv = jnp.dot(normed, w_qkv, preferred_element_type=jnp.float32).astype(jnp.bfloat16)
    cos_full, sin_full = rotary_tables(positions, head_dim)
    local_pos = positions - me * seq_dev
    k_t, v_t = jnp.swapaxes(k_cache, 1, 2), jnp.swapaxes(v_cache, 1, 2)
    k_next, v_next, stats = attention(local_pos, qkv, cos_full, sin_full, k_t, v_t, group)
    gathered = lax.all_to_all(stats, 'sp', 0, 0, tiled=True)
    context = combine(gathered, head_dim, num_heads)
    attn_out = jnp.dot(context, w_out, preferred_element_type=jnp.float32)
    up_proj = jnp.dot(normed, w_up, preferred_element_type=jnp.float32)
    activated = jax.nn.gelu(up_proj, approximate=False).astype(jnp.bfloat16)
    mlp_part = jnp.dot(activated, w_down, preferred_element_type=jnp.float32)
    mlp_own = lax.psum_scatter(mlp_part, 'sp', scatter_dimension=0, tiled=True)
    out_all = lax.all_gather(attn_out + mlp_own, 'sp', axis=0, tiled=True)
    out_hidden = (hidden.astype(jnp.float32) + out_all).astype(jnp.bfloat16)
    return out_hidden, jnp.swapaxes(k_next, 1, 2), jnp.swapaxes(v_next, 1, 2)


def solution(mesh):
    cache_spec = P('dp', 'sp', None)
    in_specs = (P('dp', None), P(None), P(None), P(None, None), P(None, None), P(None, 'sp'), P('sp', None), cache_spec, cache_spec, P('dp'))
    out_specs = (P('dp', None), cache_spec, cache_spec)
    return jax.shard_map(device_step, mesh=mesh, in_specs=in_specs, out_specs=out_specs, check_vma=False)
```
